32 devices in a mesh: image: 2 (over x), band: 16 (over z, y, core).
Axes of the slice: x: 2, y: 2, z: 4, core: 2. Of those that a mesh axis runs over, the one named last changes fastest.
Arguments:
- orbitals: bfloat16 [32, 64, 4096], P(('image', 'band')), parts along dimension 0, may hold values from -6 to 6
- kernel: float32 [128, 4096], P('image'), parts along dimension 0, may hold values from 0.05 to 1
Outputs:
- exchange: bfloat16 [32, 64, 4096], P(('image', 'band')), parts along dimension 0
- energy: float32 [2], P('image'), parts along dimension 0
The draws below stay inside these ranges and needn't reach their ends.
There are 2 independent parts, one for each index of `image`. The reference program is written for one: setup_inputs(seed, part) draws one part's arguments, and reference() takes and returns one part's arrays. A program takes and returns all parts, laid end to end along the dimension named above; each array names one. Nothing has to cross between parts.
All inputs are finite; a program needn't handle non-finite values.
Results may differ from the reference program's by a relative error of at most 0.009.
Values may be sent and summed in bfloat16 or wider, within the bound.
A program may use at most 64 MiB of HBM per device.

```python
import math
import jax
import jax.numpy as jnp
from jax import lax

GRID = 64
B_DEV = 1
STEPS = 3
BANDS = 16
N_BAND = 16


def draw_orbitals(key, part):
    band_scale = 0.5 + 0.5 * jnp.arange(BANDS, dtype=jnp.float32) / max(BANDS - 1, 1)
    band_scale = band_scale[:, None, None]
    values = jax.random.normal(jax.random.fold_in(key, 7), (BANDS, GRID, GRID * GRID), jnp.float32)
    values = jnp.clip(values * band_scale, -6.0, 6.0)
    return values.astype(jnp.bfloat16)


def setup_inputs(seed: int = 0, part: int = 0) -> dict:
    streams_of = jax.random.split(jax.random.key(seed), 3)
    part_splits = jax.random.split(jax.random.fold_in(streams_of[2], part), 3)
    orbitals = draw_orbitals(jax.random.fold_in(jax.random.fold_in(streams_of[2], part), 71), part)
    kernel = jnp.clip(jnp.exp(jax.random.uniform(part_splits[1], (GRID, GRID * GRID), jnp.float32, math.log(0.05), math.log(1.0))), 0.05, 1.0)
    return {"orbitals": orbitals, "kernel": kernel}


def cas_table(length):
    wave_index = jnp.arange(length, dtype=jnp.int32)
    phase_index = wave_index[:, None] * wave_index[None, :] % length
    angles = phase_index.astype(jnp.float32) * (2.0 * math.pi / length)
    return ((jnp.cos(angles) + jnp.sin(angles)) / math.sqrt(length)).astype(jnp.bfloat16)

def apply_pass(form, field, cas):
    return jnp.einsum(form, field.astype(jnp.float32), cas.astype(jnp.float32), precision=lax.Precision.HIGHEST).astype(jnp.bfloat16)

def transform(field, cas):
    field = apply_pass('pabc,cz->pabz', field, cas)
    field = apply_pass('pabz,by->payz', field, cas)
    return apply_pass('payz,ax->pxyz', field, cas)

def potentials(mine, other, kernel_cube, cas):
    count_a, count_b = (mine.shape[0], other.shape[0])
    density = (mine[:, None].astype(jnp.float32) * other[None].astype(jnp.float32)).astype(jnp.bfloat16)
    density = density.reshape((count_a * count_b,) + mine.shape[1:])
    spectral = transform(density, cas)
    weighted = (kernel_cube[None] * spectral.astype(jnp.float32)).astype(jnp.bfloat16)
    return transform(weighted, cas).reshape((count_a, count_b) + mine.shape[1:])

def reference(orbitals, kernel):
    blocks = orbitals.reshape(N_BAND, B_DEV, GRID, GRID, GRID)
    kernel_cube = kernel.reshape(GRID, GRID, GRID)
    cas = cas_table(GRID)

    def per_block(index):
        mine = lax.dynamic_index_in_dim(blocks, index, 0, keepdims=False)
        collected = jnp.zeros(mine.shape, jnp.float32)
        for offset in range(-STEPS, STEPS + 1):
            where = ((index + offset + N_BAND) % N_BAND).astype(jnp.int32)
            other = lax.dynamic_index_in_dim(blocks, where, 0, keepdims=False)
            pot = potentials(mine, other, kernel_cube, cas)
            collected = collected - jnp.einsum('ijxyz,jxyz->ixyz', pot.astype(jnp.float32), other.astype(jnp.float32), precision=lax.Precision.HIGHEST)
        part_energy = 0.5 * jnp.sum(mine.astype(jnp.float32) * collected) / float(GRID ** 3)
        return (collected.astype(jnp.bfloat16), part_energy)
    exchange, parts = lax.map(per_block, jnp.arange(N_BAND, dtype=jnp.int32))
    return (exchange.reshape(orbitals.shape), jnp.sum(parts).reshape(1))
```

```python
import functools

import jax
import jax.numpy as jnp
import numpy as np
from jax import lax
from jax.experimental import pallas as pl
from jax.experimental.pallas import tpu as pltpu
from jax.sharding import PartitionSpec as P

MESH = pl.DeviceIdType.MESH
F32 = jnp.float32
BF16 = jnp.bfloat16


def cas_table(length):
    wave_index = np.arange(length, dtype=np.int32)
    phase_index = wave_index[:, None] * wave_index[None, :] % length
    angles = phase_index.astype(np.float32) * np.float32(2.0 * np.pi / length)
    table = (np.cos(angles) + np.sin(angles)) / np.float32(np.sqrt(length))
    return table.astype(np.float32)


def dot(a, b):
    return jnp.dot(a, b, preferred_element_type=F32)


def split_halves(low, high, g):
    lane = lax.broadcasted_iota(jnp.int32, low.shape, 1)
    first = jnp.concatenate([low[:, :g], high[:, :g]], axis=1)
    second = jnp.concatenate([low[:, g:], high[:, g:]], axis=1)
    del lane
    return first, second


def kernel(n, g, orb, vin, hx, hy, out, en, slots, vdup, mdup, pack, t1, t2, acc,
           e_own, e_all, send_sem, recv_sem, e_send, e_recv):
    me = lax.axis_index("band")
    odd = lax.rem(me, 2)
    at = lambda d: lax.rem(me + d + n, n)
    partner = at(1 - 2 * odd)
    up, down = at(2), at(-2)
    far = at(6 * odd - 3)
    to = lambda b: {"band": b}

    barrier = pltpu.get_barrier_semaphore()

    @pl.loop(1, n)
    def _(d):
        pl.semaphore_signal(barrier, inc=1, device_id=to(lax.rem(me + d, n)), device_id_type=MESH)

    pl.semaphore_wait(barrier, n - 1)

    def copy(k, src, dst):
        return pltpu.make_async_remote_copy(
            src_ref=src, dst_ref=slots.at[k], send_sem=send_sem.at[k], recv_sem=recv_sem.at[k],
            device_id=to(dst), device_id_type=MESH)

    copies = [copy(0, orb, partner), copy(1, orb, up), copy(2, orb, down), copy(3, orb, far),
              copy(4, slots.at[1], partner), copy(5, slots.at[2], partner)]
    for k in (1, 2, 3, 0):
        copies[k].start()

    half = g // 2
    xh_n = g // 8

    @pl.loop(0, half)
    def _(t):
        c = pl.ds(pl.multiple_of(t * 2 * g, 2 * g), 2 * g)
        m = orb[:, c]
        a, b = split_halves(m, m, g)
        mdup[2 * t] = a
        mdup[2 * t + 1] = b
        v = vin[:, c]
        a, b = split_halves(v, v, g)
        for xh in range(xh_n):
            r = slice(xh * 8, xh * 8 + 8)
            vdup[xh, pl.ds(pl.multiple_of(t * 16, 16), 8), :] = a[r]
            vdup[xh, pl.ds(pl.multiple_of(t * 16 + 8, 8), 8), :] = b[r]

    def tiles(ref, yg):
        parts = [ref[pl.ds(yg * 8 + ya * 4, 4)].reshape(4 * g, 2 * g) for ya in range(2)]
        return jnp.concatenate(parts, axis=1)

    def group(a_ref, b_ref, first):
        @pl.loop(0, half)
        def _(t):
            c = pl.ds(pl.multiple_of(t * 2 * g, 2 * g), 2 * g)
            a = a_ref[:, c]
            b = jnp.zeros_like(a) if b_ref is None else b_ref[:, c]
            p, q = split_halves(a, b, g)
            pack[2 * t] = p
            pack[2 * t + 1] = q

        @pl.loop(0, g // 8, unroll=2)
        def _(yg):
            d = tiles(mdup, yg) * tiles(pack, yg)
            h = hx[...]
            u = dot(h, d).astype(BF16)
            u = dot(u, h).reshape(4, xh_n, 8, 4 * g)
            for xh in range(xh_n):
                for ya in range(2):
                    piece = u[:, xh, :, ya * 2 * g:(ya + 1) * 2 * g].reshape(32, 2 * g)
                    rows = pl.ds(pl.multiple_of(yg * 64 + ya * 32, 32), 32)
                    t1[xh, rows, :] = piece.astype(BF16)

        @pl.loop(0, xh_n // 2)
        def _(xg):
            w = jnp.concatenate([t1[2 * xg], t1[2 * xg + 1]], axis=1)
            v = jnp.concatenate([vdup[2 * xg], vdup[2 * xg + 1]], axis=1)
            k = hy[...]
            w = (dot(k, w) * v).astype(BF16)
            w = dot(k, w).reshape(g, 8, 4 * g)
            w = jnp.concatenate([w[:, :, :2 * g], w[:, :, 2 * g:]], axis=1)
            t2[:, pl.ds(pl.multiple_of(xg * 16, 16), 16), :] = w.astype(BF16)

        @pl.loop(0, g // 8, unroll=2)
        def _(yg):
            h = hx[...]
            u = dot(tiles(t2, yg), h).astype(BF16)
            u = dot(h, u) * tiles(pack, yg).astype(F32)
            for ya in range(2):
                y = pl.ds(yg * 8 + ya * 4, 4)
                piece = u[:, ya * 2 * g:(ya + 1) * 2 * g].reshape(4, g, 2 * g)
                acc[y] = piece if first else acc[y] + piece

    copies[0].wait_recv()
    group(orb, slots.at[0], True)
    copies[1].wait_recv()
    copies[4].start()
    copies[2].wait_recv()
    copies[5].start()
    group(slots.at[1], slots.at[2], False)
    copies[4].wait_recv()
    copies[5].wait_recv()
    group(slots.at[4], slots.at[5], False)
    copies[3].wait_recv()
    group(slots.at[3], None, False)

    e_own[...] = jnp.zeros_like(e_own)

    @pl.loop(0, half)
    def _(t):
        c = pl.ds(pl.multiple_of(t * 2 * g, 2 * g), 2 * g)
        e = acc[2 * t]
        o = acc[2 * t + 1]
        total = -jnp.concatenate([e[:, :g] + e[:, g:], o[:, :g] + o[:, g:]], axis=1)
        out[:, c] = total.astype(BF16)
        s = total * orb[:, c].astype(F32)
        e_own[...] += jnp.sum(s.reshape(g // 8, 8, 2 * g), axis=0)

    def share(d):
        there = lax.rem(me + d, n)
        return pltpu.make_async_remote_copy(
            src_ref=e_own, dst_ref=e_all.at[d], send_sem=e_send.at[d], recv_sem=e_recv.at[d],
            device_id=to(there), device_id_type=MESH)

    @pl.loop(1, n)
    def _(d):
        share(d).start()

    for k in range(6):
        copies[k].wait_send()

    e_all[0] = e_own[...]

    @pl.loop(1, n)
    def _(d):
        share(d).wait()

    en[0] = 0.5 * jnp.sum(jnp.sum(e_all[...], axis=0)) / float(g ** 3)


def shards(orbitals, weights):
    _, g, area = orbitals.shape
    n = lax.axis_size("band")
    table = cas_table(g)
    hx = jnp.asarray(np.kron(np.eye(4, dtype=np.float32), table), BF16)
    hy = jnp.asarray(np.kron(table, np.eye(8, dtype=np.float32)), BF16)
    vm = pl.BlockSpec(memory_space=pltpu.VMEM)
    exchange, energy = pl.pallas_call(
        functools.partial(kernel, n, g),
        out_shape=(jax.ShapeDtypeStruct((g, area), BF16), jax.ShapeDtypeStruct((1,), F32)),
        in_specs=[vm] * 4,
        out_specs=(vm, pl.BlockSpec(memory_space=pltpu.SMEM)),
        scratch_shapes=[
            pltpu.VMEM((6, g, area), BF16),
            pltpu.VMEM((g // 8, 8 * g, 2 * g), F32),
            pltpu.VMEM((g, g, 2 * g), BF16),
            pltpu.VMEM((g, g, 2 * g), BF16),
            pltpu.VMEM((g // 8, 8 * g, 2 * g), BF16),
            pltpu.VMEM((g, g, 2 * g), BF16),
            pltpu.VMEM((g, g, 2 * g), F32),
            pltpu.VMEM((8, 2 * g), F32),
            pltpu.VMEM((n, 8, 2 * g), F32),
            pltpu.SemaphoreType.DMA((6,)),
            pltpu.SemaphoreType.DMA((6,)),
            pltpu.SemaphoreType.DMA((n,)),
            pltpu.SemaphoreType.DMA((n,)),
        ],
        compiler_params=pltpu.CompilerParams(
            collective_id=0, has_side_effects=True, vmem_limit_bytes=48 * 1024 * 1024),
    )(orbitals.reshape(g, area), weights, hx, hy)
    return exchange.reshape(orbitals.shape), energy


def solution(mesh):
    in_specs = (P(("image", "band"), None, None), P("image", None))
    out_specs = (P(("image", "band"), None, None), P("image"))
    return jax.shard_map(shards, mesh=mesh, in_specs=in_specs, out_specs=out_specs, check_vma=False)
```

```python
import functools

import jax
import jax.numpy as jnp
import numpy as np
from jax import lax
from jax.experimental import pallas as pl
from jax.experimental.pallas import tpu as pltpu
from jax.sharding import PartitionSpec as P

CHUNKS = 4
MESH = pl.DeviceIdType.MESH
F32 = jnp.float32
BF16 = jnp.bfloat16


def cas_table(length):
    wave_index = np.arange(length, dtype=np.int32)
    phase_index = wave_index[:, None] * wave_index[None, :] % length
    angles = phase_index.astype(np.float32) * np.float32(2.0 * np.pi / length)
    table = (np.cos(angles) + np.sin(angles)) / np.float32(np.sqrt(length))
    return table.astype(np.float32)


def dot(a, b):
    return jnp.dot(a, b, preferred_element_type=F32)


def split_halves(low, high, g):
    first = jnp.concatenate([low[:, :g], high[:, :g]], axis=1)
    second = jnp.concatenate([low[:, g:], high[:, g:]], axis=1)
    return first, second


def kernel(n, g, orb_hbm, vin_hbm, hx_hbm, hy_hbm, out, en, orb, vin, hx, hy, slots, vdup, mdup,
           pack, t1, t2, acc, e_own, e_all, in_sem, send_sem, recv_sem, e_send, e_recv):
    me = lax.axis_index("band")
    core = lax.rem(me, 2)
    side = 1 - 2 * lax.rem(me // 2, 2)
    at = lambda d: lax.rem(me + d + n, n)
    partner = at(1 - 2 * core)
    near = at(2 * side)
    beyond = at(4 * side)
    far = at(6 * core - 3)
    to = lambda b: {"band": b}

    loads = [pltpu.make_async_copy(src, dst, in_sem.at[i]) for i, (src, dst) in enumerate(
        ((orb_hbm, orb), (vin_hbm, vin), (hx_hbm, hx), (hy_hbm, hy)))]
    for load in loads:
        load.start()

    barrier = pltpu.get_barrier_semaphore()

    @pl.loop(1, n)
    def _(d):
        pl.semaphore_signal(barrier, inc=1, device_id=to(lax.rem(me + d, n)), device_id_type=MESH)

    loads[0].wait()
    pl.semaphore_wait(barrier, n - 1)

    rows = g // CHUNKS

    def copies(k, src, dst):
        return [pltpu.make_async_remote_copy(
            src_ref=src.at[pl.ds(i * rows, rows)], dst_ref=slots.at[k, pl.ds(i * rows, rows)],
            send_sem=send_sem.at[k, i], recv_sem=recv_sem.at[k, i],
            device_id=to(dst), device_id_type=MESH) for i in range(CHUNKS)]

    to_partner = copies(0, orb, partner)
    to_near = copies(1, orb, near)
    relayed = copies(2, slots.at[1], beyond)
    to_far = copies(3, orb, far)
    pass_near = copies(4, slots.at[1], partner)
    pass_relayed = copies(5, slots.at[2], partner)
    for group_of in (to_near, to_far, to_partner):
        for c in group_of:
            c.start()

    def relay_near(i):
        to_near[i].wait_recv()
        relayed[i].start()
        pass_near[i].start()

    def relay_far(i):
        relayed[i].wait_recv()
        pass_relayed[i].start()

    def arrived(group_of):
        for c in group_of:
            c.wait_recv()

    for load in loads[1:]:
        load.wait()

    half = g // 2
    xh_n = g // 8

    @pl.loop(0, half, unroll=8)
    def _(t):
        c = pl.ds(pl.multiple_of(t * 2 * g, 2 * g), 2 * g)
        m = orb[:, c]
        a, b = split_halves(m, m, g)
        mdup[2 * t] = a
        mdup[2 * t + 1] = b
        v = vin[:, c]
        a, b = split_halves(v, v, g)
        for xh in range(xh_n):
            r = slice(xh * 8, xh * 8 + 8)
            vdup[xh, pl.ds(pl.multiple_of(t * 16, 16), 8), :] = a[r]
            vdup[xh, pl.ds(pl.multiple_of(t * 16 + 8, 8), 8), :] = b[r]

    def tiles(ref, yg):
        parts = [ref[pl.ds(yg * 8 + ya * 4, 4)].reshape(4 * g, 2 * g) for ya in range(2)]
        return jnp.concatenate(parts, axis=1)

    def group(a_ref, b_ref, first, hook1, hook2):
        @pl.loop(0, half, unroll=8)
        def _(t):
            c = pl.ds(pl.multiple_of(t * 2 * g, 2 * g), 2 * g)
            a = a_ref[:, c]
            b = jnp.zeros_like(a) if b_ref is None else b_ref[:, c]
            p, q = split_halves(a, b, g)
            pack[2 * t] = p
            pack[2 * t + 1] = q

        @pl.loop(0, g // 8, unroll=8)
        def _(yg):
            d = tiles(mdup, yg) * tiles(pack, yg)
            h = hx[...]
            u = dot(h, d).astype(BF16)
            u = dot(u, h).reshape(4, xh_n, 8, 4 * g)
            for xh in range(xh_n):
                for ya in range(2):
                    piece = u[:, xh, :, ya * 2 * g:(ya + 1) * 2 * g].reshape(32, 2 * g)
                    rows = pl.ds(pl.multiple_of(yg * 64 + ya * 32, 32), 32)
                    t1[xh, rows, :] = piece.astype(BF16)

        hook1()

        @pl.loop(0, xh_n // 2, unroll=4)
        def _(xg):
            w = jnp.concatenate([t1[2 * xg], t1[2 * xg + 1]], axis=1)
            v = jnp.concatenate([vdup[2 * xg], vdup[2 * xg + 1]], axis=1)
            k = hy[...]
            w = (dot(k, w) * v).astype(BF16)
            w = dot(k, w).reshape(g, 8, 4 * g)
            w = jnp.concatenate([w[:, :, :2 * g], w[:, :, 2 * g:]], axis=1)
            t2[:, pl.ds(pl.multiple_of(xg * 16, 16), 16), :] = w.astype(BF16)

        hook2()

        @pl.loop(0, g // 8, unroll=8)
        def _(yg):
            h = hx[...]
            u = dot(tiles(t2, yg), h).astype(BF16)
            u = dot(h, u) * tiles(pack, yg).astype(F32)
            for ya in range(2):
                y = pl.ds(yg * 8 + ya * 4, 4)
                piece = u[:, ya * 2 * g:(ya + 1) * 2 * g].reshape(4, g, 2 * g)
                acc[y] = piece if first else acc[y] + piece

    arrived(to_partner)
    group(orb, slots.at[0], True, lambda: relay_near(0), lambda: relay_near(1))
    arrived(to_far)
    group(slots.at[3], None, False, lambda: relay_near(2), lambda: None)
    relay_near(3)
    arrived(pass_near)
    group(slots.at[1], slots.at[4], False, lambda: relay_far(0), lambda: relay_far(1))
    relay_far(2)
    relay_far(3)
    arrived(pass_relayed)
    group(slots.at[2], slots.at[5], False, lambda: None, lambda: None)

    e_own[...] = jnp.zeros_like(e_own)

    @pl.loop(0, half, unroll=8)
    def _(t):
        c = pl.ds(pl.multiple_of(t * 2 * g, 2 * g), 2 * g)
        e = acc[2 * t]
        o = acc[2 * t + 1]
        total = -jnp.concatenate([e[:, :g] + e[:, g:], o[:, :g] + o[:, g:]], axis=1)
        out[:, c] = total.astype(BF16)
        s = total * orb[:, c].astype(F32)
        e_own[...] += jnp.sum(s.reshape(g // 8, 8, 2 * g), axis=0)

    def share(d):
        there = lax.rem(me + d, n)
        return pltpu.make_async_remote_copy(
            src_ref=e_own, dst_ref=e_all.at[d], send_sem=e_send.at[d], recv_sem=e_recv.at[d],
            device_id=to(there), device_id_type=MESH)

    @pl.loop(1, n)
    def _(d):
        share(d).start()

    for group_of in (to_partner, to_near, relayed, to_far, pass_near, pass_relayed):
        for c in group_of:
            c.wait_send()

    e_all[0] = e_own[...]

    @pl.loop(1, n)
    def _(d):
        share(d).wait()

    en[0] = 0.5 * jnp.sum(jnp.sum(e_all[...], axis=0)) / float(g ** 3)


def shards(orbitals, weights):
    _, g, area = orbitals.shape
    n = lax.axis_size("band")
    table = cas_table(g)
    hx = jnp.asarray(np.kron(np.eye(4, dtype=np.float32), table), BF16)
    hy = jnp.asarray(np.kron(table, np.eye(8, dtype=np.float32)), BF16)
    vm = pl.BlockSpec(memory_space=pltpu.VMEM)
    exchange, energy = pl.pallas_call(
        functools.partial(kernel, n, g),
        out_shape=(jax.ShapeDtypeStruct((g, area), BF16), jax.ShapeDtypeStruct((1,), F32)),
        in_specs=[pl.BlockSpec(memory_space=pl.ANY)] * 4,
        out_specs=(vm, pl.BlockSpec(memory_space=pltpu.SMEM)),
        scratch_shapes=[
            pltpu.VMEM((g, area), BF16),
            pltpu.VMEM((g, area), F32),
            pltpu.VMEM(hx.shape, BF16),
            pltpu.VMEM(hy.shape, BF16),
            pltpu.VMEM((6, g, area), BF16),
            pltpu.VMEM((g // 8, 8 * g, 2 * g), F32),
            pltpu.VMEM((g, g, 2 * g), BF16),
            pltpu.VMEM((g, g, 2 * g), BF16),
            pltpu.VMEM((g // 8, 8 * g, 2 * g), BF16),
            pltpu.VMEM((g, g, 2 * g), BF16),
            pltpu.VMEM((g, g, 2 * g), F32),
            pltpu.VMEM((8, 2 * g), F32),
            pltpu.VMEM((n, 8, 2 * g), F32),
            pltpu.SemaphoreType.DMA((4,)),
            pltpu.SemaphoreType.DMA((6, CHUNKS)),
            pltpu.SemaphoreType.DMA((6, CHUNKS)),
            pltpu.SemaphoreType.DMA((n,)),
            pltpu.SemaphoreType.DMA((n,)),
        ],
        compiler_params=pltpu.CompilerParams(
            collective_id=0, has_side_effects=True, vmem_limit_bytes=60 * 1024 * 1024),
    )(orbitals.reshape(g, area), weights, hx, hy)
    return exchange.reshape(orbitals.shape), energy


def solution(mesh):
    in_specs = (P(("image", "band"), None, None), P("image", None))
    out_specs = (P(("image", "band"), None, None), P("image"))
    return jax.shard_map(shards, mesh=mesh, in_specs=in_specs, out_specs=out_specs, check_vma=False)
```

```python
import functools

import jax
import jax.numpy as jnp
import numpy as np
from jax import lax
from jax.experimental import pallas as pl
from jax.experimental.pallas import tpu as pltpu
from jax.sharding import PartitionSpec as P

CHUNKS = 4
MESH = pl.DeviceIdType.MESH
F32 = jnp.float32
BF16 = jnp.bfloat16


def cas_table(length):
    wave_index = np.arange(length, dtype=np.int32)
    phase_index = wave_index[:, None] * wave_index[None, :] % length
    angles = phase_index.astype(np.float32) * np.float32(2.0 * np.pi / length)
    table = (np.cos(angles) + np.sin(angles)) / np.float32(np.sqrt(length))
    return table.astype(np.float32)


def dot(a, b):
    return jnp.dot(a, b, preferred_element_type=F32)


def split_halves(low, high, g):
    first = jnp.concatenate([low[:, :g], high[:, :g]], axis=1)
    second = jnp.concatenate([low[:, g:], high[:, g:]], axis=1)
    return first, second


def kernel(n, g, orb_hbm, vin_hbm, hx_hbm, hy_hbm, out, en, orb, vin, hx, hy, slots, vdup, mdup,
           pack, t1, t2, acc, e_own, e_all, in_sem, send_sem, recv_sem, e_send, e_recv):
    me = lax.axis_index("band")
    core = lax.rem(me, 2)
    side = 1 - 2 * lax.rem(me // 2, 2)
    at = lambda d: lax.rem(me + d + n, n)
    partner = at(1 - 2 * core)
    near = at(2 * side)
    beyond = at(4 * side)
    far, beside = at(3 * side), at(side)
    sends_far = lax.rem(core + lax.rem(me // 2, 2), 2) == 1
    to = lambda b: {"band": b}

    loads = [pltpu.make_async_copy(src, dst, in_sem.at[i]) for i, (src, dst) in enumerate(
        ((orb_hbm, orb), (vin_hbm, vin), (hx_hbm, hx), (hy_hbm, hy)))]
    for load in loads:
        load.start()

    barrier = pltpu.get_barrier_semaphore()

    @pl.loop(1, n)
    def _(d):
        pl.semaphore_signal(barrier, inc=1, device_id=to(lax.rem(me + d, n)), device_id_type=MESH)

    loads[0].wait()
    pl.semaphore_wait(barrier, n - 1)

    wide = g * g // CHUNKS

    def copies(k, src, dst, send):
        columns = [pl.ds(i * wide, wide) for i in range(CHUNKS)]
        return [pltpu.make_async_remote_copy(
            src_ref=src.at[:, c], dst_ref=slots.at[k, :, c],
            send_sem=send_sem.at[send, i], recv_sem=recv_sem.at[k, i],
            device_id=to(dst), device_id_type=MESH) for i, c in enumerate(columns)]

    to_partner = copies(0, orb, partner, 0)
    to_near = copies(1, orb, near, 1)
    relayed = copies(2, slots.at[1], beyond, 2)
    to_far = copies(3, orb, far, 3)
    pass_near = copies(4, slots.at[1], partner, 4)
    pass_relayed = copies(5, slots.at[2], partner, 5)
    to_beside = copies(3, slots.at[2], beside, 6)

    for c in to_near:
        c.start()

    @pl.when(sends_far)
    def _():
        for c in to_far[:2]:
            c.start()

    for c in to_partner:
        c.start()

    def relay_near(i):
        to_near[i].wait_recv()
        relayed[i].start()
        pass_near[i].start()
        if i >= 2:
            @pl.when(sends_far)
            def _():
                to_far[i].start()

    def relay_far(i):
        relayed[i].wait_recv()
        pass_relayed[i].start()

        @pl.when(sends_far)
        def _():
            to_beside[i].start()

    for load in loads[1:]:
        load.wait()

    half = g // 2
    xh_n = g // 8

    @pl.loop(0, half, unroll=8)
    def _(t):
        c = pl.ds(pl.multiple_of(t * 2 * g, 2 * g), 2 * g)
        m = orb[:, c]
        a, b = split_halves(m, m, g)
        mdup[2 * t] = a
        mdup[2 * t + 1] = b
        v = vin[:, c]
        a, b = split_halves(v, v, g)
        for xh in range(xh_n):
            r = slice(xh * 8, xh * 8 + 8)
            vdup[xh, pl.ds(pl.multiple_of(t * 16, 16), 8), :] = a[r]
            vdup[xh, pl.ds(pl.multiple_of(t * 16 + 8, 8), 8), :] = b[r]

    def tiles(ref, yg):
        parts = [ref[pl.ds(yg * 8 + ya * 4, 4)].reshape(4 * g, 2 * g) for ya in range(2)]
        return jnp.concatenate(parts, axis=1)

    def group(a_ref, b_ref, first, ready, hook1, hook2):
        for i in range(CHUNKS):
            ready(i)

            @pl.loop(i * half // CHUNKS, (i + 1) * half // CHUNKS, unroll=half // CHUNKS)
            def _(t):
                c = pl.ds(pl.multiple_of(t * 2 * g, 2 * g), 2 * g)
                a = a_ref[:, c]
                b = jnp.zeros_like(a) if b_ref is None else b_ref[:, c]
                p, q = split_halves(a, b, g)
                pack[2 * t] = p
                pack[2 * t + 1] = q

            @pl.loop(i * g // 8 // CHUNKS, (i + 1) * g // 8 // CHUNKS, unroll=g // 8 // CHUNKS)
            def _(yg):
                d = tiles(mdup, yg) * tiles(pack, yg)
                h = hx[...]
                u = dot(h, d).astype(BF16)
                u = dot(u, h).reshape(4, xh_n, 8, 4 * g)
                for xh in range(xh_n):
                    for ya in range(2):
                        piece = u[:, xh, :, ya * 2 * g:(ya + 1) * 2 * g].reshape(32, 2 * g)
                        rows = pl.ds(pl.multiple_of(yg * 64 + ya * 32, 32), 32)
                        t1[xh, rows, :] = piece.astype(BF16)

        hook1()

        @pl.loop(0, xh_n // 2, unroll=4)
        def _(xg):
            w = jnp.concatenate([t1[2 * xg], t1[2 * xg + 1]], axis=1)
            v = jnp.concatenate([vdup[2 * xg], vdup[2 * xg + 1]], axis=1)
            k = hy[...]
            w = (dot(k, w) * v).astype(BF16)
            w = dot(k, w).reshape(g, 8, 4 * g)
            w = jnp.concatenate([w[:, :, :2 * g], w[:, :, 2 * g:]], axis=1)
            t2[:, pl.ds(pl.multiple_of(xg * 16, 16), 16), :] = w.astype(BF16)

        hook2()

        @pl.loop(0, g // 8, unroll=8)
        def _(yg):
            h = hx[...]
            u = dot(tiles(t2, yg), h).astype(BF16)
            u = dot(h, u) * tiles(pack, yg).astype(F32)
            for ya in range(2):
                y = pl.ds(yg * 8 + ya * 4, 4)
                piece = u[:, ya * 2 * g:(ya + 1) * 2 * g].reshape(4, g, 2 * g)
                acc[y] = piece if first else acc[y] + piece

    def ready_near(i):
        if i >= 2:
            relay_near(i)
        pass_near[i].wait_recv()

    def ready_relayed(i):
        if i >= 3:
            relay_far(i)
        pass_relayed[i].wait_recv()

    def far_hook():
        relay_far(0)
        relay_far(1)

    group(orb, slots.at[0], True, lambda i: to_partner[i].wait_recv(),
          lambda: relay_near(0), lambda: relay_near(1))
    group(slots.at[1], slots.at[4], False, ready_near, far_hook, lambda: relay_far(2))
    group(slots.at[2], slots.at[5], False, ready_relayed, lambda: None, lambda: None)
    group(slots.at[3], None, False, lambda i: to_far[i].wait_recv(), lambda: None, lambda: None)

    e_own[...] = jnp.zeros_like(e_own)

    @pl.loop(0, half, unroll=8)
    def _(t):
        c = pl.ds(pl.multiple_of(t * 2 * g, 2 * g), 2 * g)
        e = acc[2 * t]
        o = acc[2 * t + 1]
        total = -jnp.concatenate([e[:, :g] + e[:, g:], o[:, :g] + o[:, g:]], axis=1)
        out[:, c] = total.astype(BF16)
        s = total * orb[:, c].astype(F32)
        e_own[...] += jnp.sum(s.reshape(g // 8, 8, 2 * g), axis=0)

    def share(d):
        there = lax.rem(me + d, n)
        return pltpu.make_async_remote_copy(
            src_ref=e_own, dst_ref=e_all.at[d], send_sem=e_send.at[d], recv_sem=e_recv.at[d],
            device_id=to(there), device_id_type=MESH)

    @pl.loop(1, n)
    def _(d):
        share(d).start()

    for sent in (to_partner, to_near, relayed, pass_near, pass_relayed):
        for c in sent:
            c.wait_send()

    @pl.when(sends_far)
    def _():
        for c in to_far + to_beside:
            c.wait_send()

    e_all[0] = e_own[...]

    @pl.loop(1, n)
    def _(d):
        share(d).wait()

    en[0] = 0.5 * jnp.sum(jnp.sum(e_all[...], axis=0)) / float(g ** 3)


def shards(orbitals, weights):
    _, g, area = orbitals.shape
    n = lax.axis_size("band")
    table = cas_table(g)
    hx = jnp.asarray(np.kron(np.eye(4, dtype=np.float32), table), BF16)
    hy = jnp.asarray(np.kron(table, np.eye(8, dtype=np.float32)), BF16)
    vm = pl.BlockSpec(memory_space=pltpu.VMEM)
    exchange, energy = pl.pallas_call(
        functools.partial(kernel, n, g),
        out_shape=(jax.ShapeDtypeStruct((g, area), BF16), jax.ShapeDtypeStruct((1,), F32)),
        in_specs=[pl.BlockSpec(memory_space=pl.ANY)] * 4,
        out_specs=(vm, pl.BlockSpec(memory_space=pltpu.SMEM)),
        scratch_shapes=[
            pltpu.VMEM((g, area), BF16),
            pltpu.VMEM((g, area), F32),
            pltpu.VMEM(hx.shape, BF16),
            pltpu.VMEM(hy.shape, BF16),
            pltpu.VMEM((6, g, area), BF16),
            pltpu.VMEM((g // 8, 8 * g, 2 * g), F32),
            pltpu.VMEM((g, g, 2 * g), BF16),
            pltpu.VMEM((g, g, 2 * g), BF16),
            pltpu.VMEM((g // 8, 8 * g, 2 * g), BF16),
            pltpu.VMEM((g, g, 2 * g), BF16),
            pltpu.VMEM((g, g, 2 * g), F32),
            pltpu.VMEM((8, 2 * g), F32),
            pltpu.VMEM((n, 8, 2 * g), F32),
            pltpu.SemaphoreType.DMA((4,)),
            pltpu.SemaphoreType.DMA((7, CHUNKS)),
            pltpu.SemaphoreType.DMA((6, CHUNKS)),
            pltpu.SemaphoreType.DMA((n,)),
            pltpu.SemaphoreType.DMA((n,)),
        ],
        compiler_params=pltpu.CompilerParams(
            collective_id=0, has_side_effects=True, vmem_limit_bytes=60 * 1024 * 1024),
    )(orbitals.reshape(g, area), weights, hx, hy)
    return exchange.reshape(orbitals.shape), energy


def solution(mesh):
    in_specs = (P(("image", "band"), None, None), P("image", None))
    out_specs = (P(("image", "band"), None, None), P("image"))
    return jax.shard_map(shards, mesh=mesh, in_specs=in_specs, out_specs=out_specs, check_vma=False)
```
